32 devices in a mesh: pass: 4 (over y, x), red: 4 (over z), grp: 2 (over core).
Axes of the slice: x: 2, y: 2, z: 4, core: 2. Of those that a mesh axis runs over, the one named last changes fastest.
Arguments:
- query_lex: bfloat16 [1536, 16384], P(None, 'red')
- query_dense: bfloat16 [1536, 4096], P(None, 'red')
- passage_lex: bfloat16 [4096, 16384], P(('pass', 'grp'), 'red'), may hold values from 0 to 0.47
- passage_dense: bfloat16 [4096, 4096], P(('pass', 'grp'), 'red'), may hold values from -1.33 to 1.33
- positives: int32 [1536], replicated, may hold values from 0 to 4095
Outputs:
- loss_rows: float32 [1536], P('red')
- grad_query_lex: float32 [1536, 16384], P(('pass', 'grp'), 'red')
- grad_query_dense: float32 [1536, 4096], P(('pass', 'grp'), 'red')
- grad_passage_lex: float32 [4096, 16384], P(('pass', 'grp'), 'red')
- grad_passage_dense: float32 [4096, 4096], P(('pass', 'grp'), 'red')
The draws below stay inside these ranges and needn't reach their ends.
All inputs are finite; a program needn't handle non-finite values.
Results may differ from the reference program's by a relative error of at most 0.0022.
Values may be sent and summed in bfloat16 or wider, within the bound.
A program may use at most 192 MiB of HBM per device.

```python
import jax
import jax.numpy as jnp
from jax import lax

VOCAB = 16384
WIDTH = 4096
QUERIES = 1536
PASSAGES = 4096


lex_scale = 0.46


dense_scale = 0.177


def lexical_row(base, index):
    row_key = jax.random.fold_in(base, index)
    mask_key, value_key = jax.random.split(row_key)
    present = jax.random.bernoulli(mask_key, 0.25, (VOCAB,)).astype(jnp.float32)
    values = jax.random.uniform(value_key, (VOCAB,), jnp.float32)
    ramp = 1.0 + 0.02 * index.astype(jnp.float32) / PASSAGES
    return present * values * lex_scale * ramp


def dense_row(base, index):
    row_key = jax.random.fold_in(base, index)
    value_key = jax.random.fold_in(row_key, 0)
    ramp = 0.75 + 0.5 * index.astype(jnp.float32) / PASSAGES
    values = jnp.clip(jax.random.normal(value_key, (WIDTH,), jnp.float32), -6.0, 6.0)
    return values * dense_scale * ramp


def draw_passage_lex(key, part):
    base = jax.random.fold_in(key, 11)
    indices = jnp.arange(PASSAGES)
    return jax.vmap(lambda index: lexical_row(base, index))(indices).astype(jnp.bfloat16)


def draw_passage_dense(key, part):
    base = jax.random.fold_in(key, 12)
    indices = jnp.arange(PASSAGES)
    return jax.vmap(lambda index: dense_row(base, index))(indices).astype(jnp.bfloat16)


def draw_query_lex(key, part):
    base = jax.random.fold_in(key, 21)
    mask_key, value_key = jax.random.split(base, 2)
    present = jax.random.bernoulli(mask_key, 0.25, (QUERIES, VOCAB)).astype(jnp.float32)
    values = jax.random.uniform(value_key, (QUERIES, VOCAB), jnp.float32)
    drawn = present * values * lex_scale
    return drawn.astype(jnp.bfloat16)


def draw_query_dense(key, part):
    base = jax.random.fold_in(key, 22)
    value_key = jax.random.fold_in(base, 0)
    drawn = jnp.clip(jax.random.normal(value_key, (QUERIES, WIDTH), jnp.float32), -6.0, 6.0) * dense_scale
    return drawn.astype(jnp.bfloat16)


def place_ends(values, own_key, smallest, high):
    longest = values.shape.index(max(values.shape))
    spots = []
    for shift in (0, 1):
        where = [jax.random.randint(jax.random.fold_in(own_key, axis), (), 0, length) for axis, length in enumerate(values.shape)]
        where[longest] = (where[longest] + shift) % values.shape[longest]
        spots.append(tuple(where))
    return values.at[spots[0]].set(smallest).at[spots[1]].set(high)


def setup_inputs(seed: int = 0) -> dict:
    splits = jax.random.split(jax.random.key(seed), 6)
    return {
        "query_lex": draw_query_lex(jax.random.fold_in(splits[5], 71), 0),
        "query_dense": draw_query_dense(jax.random.fold_in(splits[5], 71), 0),
        "passage_lex": draw_passage_lex(jax.random.fold_in(splits[5], 71), 0),
        "passage_dense": draw_passage_dense(jax.random.fold_in(splits[5], 71), 0),
        "positives": place_ends(jax.random.randint(splits[4], (QUERIES,), 0, PASSAGES), jax.random.fold_in(splits[4], 1), 0, PASSAGES - 1).astype(jnp.int32),
    }


def softmax_parts(logits):
    largest = jnp.max(logits, axis=1, keepdims=True)
    total = jnp.sum(jnp.exp(logits - largest), axis=1, keepdims=True)
    log_total = largest + jnp.log(total)
    return log_total[:, 0], jnp.exp(logits - log_total)


def reference(query_lex, query_dense, passage_lex, passage_dense, positives):
    lexical = jnp.dot(query_lex, passage_lex.T, preferred_element_type=jnp.float32)
    dense = jnp.dot(query_dense, passage_dense.T, preferred_element_type=jnp.float32)
    joined = dense + 0.3 * lexical
    columns = lax.broadcasted_iota(jnp.int32, (1, lexical.shape[1]), 1)
    target = (positives.astype(jnp.int32)[:, None] == columns).astype(jnp.float32)
    lse_joined, prob_joined = softmax_parts(joined)
    lse_dense, prob_dense = softmax_parts(dense)
    lse_lexical, prob_lexical = softmax_parts(lexical)
    pick_joined = jnp.sum(target * joined, axis=1)
    pick_dense = jnp.sum(target * dense, axis=1)
    pick_lexical = jnp.sum(target * lexical, axis=1)
    kl_dense = jnp.sum(prob_joined * (joined - dense), axis=1) - lse_joined + lse_dense
    kl_lex = jnp.sum(prob_joined * (joined - lexical), axis=1) - lse_joined + lse_lexical
    loss_rows = (lse_joined - pick_joined) + 0.5 * (lse_dense - pick_dense) + 0.5 * (lse_lexical - pick_lexical) + 0.5 * kl_dense + 0.5 * kl_lex
    grad_dense = (0.5 * prob_joined + prob_dense - 1.5 * target).astype(jnp.bfloat16)
    grad_lex = (-0.2 * prob_joined + prob_lexical - 0.8 * target).astype(jnp.bfloat16)
    grad_query_lex = jnp.dot(grad_lex, passage_lex, preferred_element_type=jnp.float32)
    grad_query_dense = jnp.dot(grad_dense, passage_dense, preferred_element_type=jnp.float32)
    grad_passage_lex = jnp.dot(grad_lex.T, query_lex, preferred_element_type=jnp.float32)
    grad_passage_dense = jnp.dot(grad_dense.T, query_dense, preferred_element_type=jnp.float32)
    return loss_rows, grad_query_lex, grad_query_dense, grad_passage_lex, grad_passage_dense
```

```python
import functools

import jax
import jax.numpy as jnp
from jax import lax
from jax.experimental import pallas as pl
from jax.experimental.pallas import tpu as pltpu
from jax.sharding import PartitionSpec as P

MESH = pl.DeviceIdType.MESH
LANES = 128
STAT_ROWS = 16
F32 = jnp.float32
BF16 = jnp.bfloat16


class Plan:
    def __init__(self, query_lex, query_dense, passage_lex):
        self.red = lax.axis_size("red")
        self.passes = lax.axis_size("pass")
        self.cores = lax.axis_size("grp")
        self.queries, self.lex = query_lex.shape
        self.dense = query_dense.shape[1]
        self.passages = passage_lex.shape[0]
        self.block = self.queries // (self.passes * self.cores)
        self.rows = LANES // self.passes
        self.half = self.block // 2
        self.groups = self.half // self.rows
        self.chunks = self.groups * self.cores
        self.bits = self.passes.bit_length() - 1
        self.plane = self.passes * self.cores
        self.tile = min(512, self.lex, self.dense)
        self.columns = self.lex + self.dense
        tiles = self.columns // self.tile
        self.edges = [(s * tiles // self.bits) * self.tile for s in range(self.bits)] + [self.columns]
        self.keep_slots = -(-self.bits // self.cores)
        assert self.passes == 1 << self.bits and self.passes > 1
        assert self.groups * self.rows * 2 == self.block
        assert self.lex % self.tile == 0 and self.dense % self.tile == 0
        self.steps = self.chunks + 2 * (self.red - 1) + self.bits + 1


def fused(
    plan,
    ql_hbm, qd_hbm, pl_hbm, pd_hbm, pos_ref,
    g_out, loss_out, gql_out, gqd_out,
    qlv, qdv, plv, pdv, rs, grad, gx, st, lossb, tsend, trecv, keep,
    q_sem, p_sem, o_sem, ps_sem, pr_sem, rss_sem, rsr_sem, sts_sem, str_sem, gs_sem, gr_sem,
    xs_sem, xr_sem, ts_sem, tr_sem, ls_sem, lr_sem,
):
    n, passes, cores, chunks, bits = plan.red, plan.passes, plan.cores, plan.chunks, plan.bits
    me = lax.axis_index("red")
    my_pass = lax.axis_index("pass")
    my_core = lax.axis_index("grp")
    place = my_pass * cores + my_core
    hops = (n - 1 - me, me)
    onward = (me - 1, me + 1)
    back = (me + 1, me - 1)

    def local_q(d, c, t):
        core, group = lax.rem(c, cores), c // cores
        source = (ql_hbm, qd_hbm)[t]
        target = (qlv, qdv)[t]
        start = d * plan.half + group * plan.rows
        return pltpu.make_async_copy(
            source.at[:, core, pl.ds(pl.multiple_of(start, plan.rows), plan.rows), :],
            target.at[d, c],
            q_sem.at[d, c, t],
        )

    def local_p(t):
        return pltpu.make_async_copy((pl_hbm, pd_hbm)[t], (plv, pdv)[t].at[my_core], p_sem.at[t])

    def send_p(k, t):
        other = lax.rem(my_core + k, cores)
        return pltpu.make_async_remote_copy(
            src_ref=(pl_hbm, pd_hbm)[t],
            dst_ref=(plv, pdv)[t].at[my_core],
            send_sem=ps_sem.at[k - 1, t],
            recv_sem=pr_sem.at[k - 1, t],
            device_id={"grp": other},
            device_id_type=MESH,
        )

    def rs_copy(d, c, t):
        return pltpu.make_async_remote_copy(
            src_ref=rs.at[d, c, t],
            dst_ref=rs.at[d, c, t],
            send_sem=rss_sem.at[d, c, t],
            recv_sem=rsr_sem.at[d, c, t],
            device_id={"red": onward[d]},
            device_id_type=MESH,
        )

    def st_copy(c, k):
        peer = lax.rem(place + k, plan.plane)
        return pltpu.make_async_remote_copy(
            src_ref=st.at[c, place],
            dst_ref=st.at[c, place],
            send_sem=sts_sem.at[c, k - 1],
            recv_sem=str_sem.at[c, k - 1],
            device_id={"pass": peer // cores, "grp": lax.rem(peer, cores)},
            device_id_type=MESH,
        )

    def g_copy(d, c):
        return pltpu.make_async_remote_copy(
            src_ref=grad.at[d, c],
            dst_ref=grad.at[d, c],
            send_sem=gs_sem.at[d, c],
            recv_sem=gr_sem.at[d, c],
            device_id={"red": back[d]},
            device_id_type=MESH,
        )

    def g_store(d, c):
        return pltpu.make_async_copy(grad.at[d, c], g_out.at[d, c], o_sem.at[d, c])

    def x_copy(d, c, slot, target):
        return pltpu.make_async_remote_copy(
            src_ref=grad.at[d, c],
            dst_ref=gx.at[d, c // cores, slot],
            send_sem=xs_sem.at[d, c],
            recv_sem=xr_sem.at[d, c // cores, slot],
            device_id={"grp": target},
            device_id_type=MESH,
        )

    def part(phase):
        start = passes - (passes >> phase)
        return start, passes >> (phase + 1)

    def t_copy(d, group, phase, s):
        first, count = part(phase)
        lo, hi = plan.edges[s], plan.edges[s + 1]
        bit = (s + phase) % bits
        mine = lax.rem(my_pass // (1 << bit), 2)
        peer = my_pass + (1 - 2 * mine) * (1 << bit)
        where = (d, group, pl.ds(first, count), slice(None), pl.ds(lo, hi - lo))
        return pltpu.make_async_remote_copy(
            src_ref=tsend.at[where],
            dst_ref=trecv.at[where],
            send_sem=ts_sem.at[d, group, phase, s],
            recv_sem=tr_sem.at[d, group, phase, s],
            device_id={"pass": peer},
            device_id_type=MESH,
        )

    def loss_copy(d, k):
        return pltpu.make_async_remote_copy(
            src_ref=lossb.at[d],
            dst_ref=lossb.at[d],
            send_sem=ls_sem.at[k - 1],
            recv_sem=lr_sem.at[d],
            device_id={"red": lax.rem(me + k, n)},
            device_id_type=MESH,
        )

    for t in range(2):
        local_p(t).start()
    for c in range(chunks):
        for d in (1, 0):
            for t in range(2):
                local_q(d, c, t).start()

    barrier = pltpu.get_barrier_semaphore()
    for k in range(1, plan.plane):
        peer = lax.rem(place + k, plan.plane)
        pl.semaphore_signal(
            barrier, inc=1,
            device_id={"pass": peer // cores, "grp": lax.rem(peer, cores)}, device_id_type=MESH,
        )
    for k in range(1, n):
        pl.semaphore_signal(barrier, inc=1, device_id={"red": lax.rem(me + k, n)}, device_id_type=MESH)
    pl.semaphore_wait(barrier, plan.plane - 1 + n - 1)

    for k in range(1, cores):
        for t in range(2):
            send_p(k, t).start()
    for t in range(2):
        local_p(t).wait()

    first_column = place * plan.passages
    column = first_column + lax.broadcasted_iota(jnp.int32, (plan.passages, LANES), 0)

    def partial_scores(d, c, t):
        local_q(d, c, t).wait()
        rows = (qlv, qdv)[t][d, c].reshape(LANES, (plan.lex, plan.dense)[t])
        total = lax.dot_general(
            (plv, pdv)[t][my_core], rows, (((1,), (1,)), ((), ())), preferred_element_type=F32
        )
        rs_now = rs.at[d, c, t]

        @pl.when(hops[d] > 0)
        def _():
            rs_copy(d, c, t).wait_recv()
            rs_now[...] += total

        @pl.when(hops[d] == 0)
        def _():
            rs_now[...] = total

        @pl.when(hops[d] < n - 1)
        def _():
            rs_copy(d, c, t).start()

    def scores_of(d, c):
        lexical, dense = rs[d, c, 0], rs[d, c, 1]
        return dense + 0.3 * lexical, dense, lexical

    def statistics(d, c):
        scores = scores_of(d, c)
        joined, dense, lexical = scores
        target = column == pos_ref[d, c]
        st_now = st.at[c, place]
        powers = []
        for i in range(3):
            largest = jnp.max(scores[i], axis=0, keepdims=True)
            power = jnp.exp(scores[i] - largest)
            powers.append(power)
            st_now[i:i + 1] = largest
            st_now[3 + i:4 + i] = jnp.sum(power, axis=0, keepdims=True)
            st_now[8 + i:9 + i] = jnp.sum(jnp.where(target, scores[i], 0.0), axis=0, keepdims=True)
        st_now[6:7] = jnp.sum(powers[0] * (joined - dense), axis=0, keepdims=True)
        st_now[7:8] = jnp.sum(powers[0] * (joined - lexical), axis=0, keepdims=True)
        st_now[11:STAT_ROWS] = jnp.zeros((STAT_ROWS - 11, LANES), F32)
        for k in range(1, plan.plane):
            st_copy(c, k).start()

    def gradients(d, c):
        for k in range(1, plan.plane):
            st_copy(c, k).wait_recv()
        everyone = st[c]
        maxima = jnp.max(everyone[:, 0:3], axis=0)
        factors = jnp.exp(everyone[:, 0:3] - maxima[None])
        totals = jnp.sum(factors * everyone[:, 3:6], axis=0)
        weighted_dense = jnp.sum(factors[:, 0:1] * everyone[:, 6:7], axis=0)
        weighted_lex = jnp.sum(factors[:, 0:1] * everyone[:, 7:8], axis=0)
        picked = jnp.sum(everyone[:, 8:11], axis=0)
        logs = maxima + jnp.log(totals)
        log_joined, log_dense, log_lex = logs[0:1], logs[1:2], logs[2:3]
        kl_dense = weighted_dense / totals[0:1] - log_joined + log_dense
        kl_lex = weighted_lex / totals[0:1] - log_joined + log_lex
        loss = (
            log_joined - picked[0:1]
            + 0.5 * (log_dense - picked[1:2])
            + 0.5 * (log_lex - picked[2:3])
            + 0.5 * kl_dense
            + 0.5 * kl_lex
        )
        lossb[d, c] = jnp.broadcast_to(loss, (8, LANES))
        joined, dense, lexical = scores_of(d, c)
        target = (column == pos_ref[d, c]).astype(F32)
        prob = jnp.exp(joined - log_joined)
        grad[d, c, 0] = (-0.2 * prob + jnp.exp(lexical - log_lex) - 0.8 * target).astype(BF16)
        grad[d, c, 1] = (0.5 * prob + jnp.exp(dense - log_dense) - 1.5 * target).astype(BF16)

    def terms(d, c):
        group = c // cores
        slot = lax.rem(group, plan.keep_slots)
        for k in range(1, cores):
            x_copy(d, c, k - 1, lax.rem(my_core + k, cores)).wait_recv()
        for t in range(2):
            base = 0 if t == 0 else plan.lex
            lefts = [(my_core, grad[d, c, t].T)]
            for k in range(1, cores):
                lefts.append((lax.rem(my_core + k, cores), gx[d, group, k - 1, t].T))
            width = (plan.lex, plan.dense)[t]
            for s in range(bits):
                lo = max(plan.edges[s], base)
                hi = min(plan.edges[s + 1], base + width)
                if lo >= hi:
                    continue

                def column_tile(i, carry, lo=lo, s=s, t=t, base=base, lefts=lefts):
                    where = pl.ds(pl.multiple_of(lo - base + i * plan.tile, plan.tile), plan.tile)
                    there = pl.ds(pl.multiple_of(lo + i * plan.tile, plan.tile), plan.tile)
                    total = None
                    for core, left in lefts:
                        term = jnp.dot(left, (plv, pdv)[t][core, :, where], preferred_element_type=F32)
                        total = term if total is None else total + term
                    blocks = total.reshape(passes, plan.rows, plan.tile)
                    bit = s % bits
                    split = blocks.reshape(passes >> (bit + 1), 2, 1 << bit, plan.rows, plan.tile)
                    mine = lax.rem(my_pass // (1 << bit), 2)
                    zero, one = split[:, 0], split[:, 1]
                    pick = mine == 0
                    kept = jnp.where(pick, zero, one).reshape(passes // 2, plan.rows, plan.tile)
                    away = jnp.where(pick, one, zero).reshape(passes // 2, plan.rows, plan.tile)
                    first, count = part(0)
                    for a in range(count):
                        source = order(s, a)
                        tsend[d, group, first + a, :, there] = away[source].astype(BF16)
                        keep[d, slot, a, :, there] = kept[source]
                    return carry

                lax.fori_loop(0, (hi - lo) // plan.tile, column_tile, 0)
        for s in range(bits):
            t_copy(d, group, 0, s).start()

    def order(s, a):
        first_bit = s % bits
        natural = [bit for bit in range(bits) if bit != first_bit]
        place_of = 0
        for step in range(1, bits):
            bit = (s + step) % bits
            place_of |= ((a >> (step - 1)) & 1) << natural.index(bit)
        return place_of

    def later_phase(d, c, phase):
        group = c // cores
        slot = lax.rem(group, plan.keep_slots)
        for s in range(bits):
            t_copy(d, group, phase - 1, s).wait_recv()
            lo, hi = plan.edges[s], plan.edges[s + 1]
            before, had = part(phase - 1)
            first, count = part(phase)
            bit = (s + phase) % bits
            mine = lax.rem(my_pass // (1 << bit), 2)

            def column_tile(i, carry, lo=lo, before=before, first=first, count=count, mine=mine):
                there = pl.ds(pl.multiple_of(lo + i * plan.tile, plan.tile), plan.tile)
                for a in range(count):
                    both = []
                    for value in range(2):
                        b = 2 * a + value
                        both.append(keep[d, slot, b, :, there] + trecv[d, group, before + b, :, there].astype(F32))
                    pick = mine == 0
                    tsend[d, group, first + a, :, there] = jnp.where(pick, both[1], both[0]).astype(BF16)
                    keep[d, slot, a, :, there] = jnp.where(pick, both[0], both[1])
                return carry

            lax.fori_loop(0, (hi - lo) // plan.tile, column_tile, 0)
            t_copy(d, group, phase, s).start()

    def finish(d, c):
        group = c // cores
        slot = lax.rem(group, plan.keep_slots)
        last, _ = part(bits - 1)
        for s in range(bits):
            t_copy(d, group, bits - 1, s).wait_recv()
        for out, base, width in ((gql_out, 0, plan.lex), (gqd_out, plan.lex, plan.dense)):

            def column_tile(i, carry, out=out, base=base):
                there = pl.ds(pl.multiple_of(base + i * plan.tile, plan.tile), plan.tile)
                where = pl.ds(pl.multiple_of(i * plan.tile, plan.tile), plan.tile)
                out[d, group, :, where] = keep[d, slot, 0, :, there] + trecv[d, group, last, :, there].astype(F32)
                return carry

            lax.fori_loop(0, width // plan.tile, column_tile, 0)

    def inside(c):
        return jnp.logical_and(c >= 0, c < chunks)

    def step(tau, carry):
        for t in range(2):
            for d in range(2):
                c = tau - hops[d]

                @pl.when(inside(c))
                def _(d=d, c=c, t=t):
                    partial_scores(d, c, t)

        for d in range(2):
            c = tau - (n - 1)

            @pl.when(jnp.logical_and(inside(c), hops[d] == n - 1))
            def _(d=d, c=c):
                statistics(d, c)
                gradients(d, c)

                @pl.when(c == chunks - 1)
                def _():
                    for k in range(1, n):
                        loss_copy(d, k).start()

        for d in range(2):
            away = n - 1 - hops[d]
            c = tau - (n - 1) - away

            @pl.when(inside(c))
            def _(d=d, c=c, away=away):
                @pl.when(away > 0)
                def _():
                    g_copy(d, c).wait_recv()

                @pl.when(away < n - 1)
                def _():
                    g_copy(d, c).start()

                g_store(d, c).start()
                core = lax.rem(c, cores)

                @pl.when(core != my_core)
                def _():
                    x_copy(d, c, lax.rem(my_core - core + cores, cores) - 1, core).start()

        def my_turn(c):
            return jnp.logical_and(inside(c), lax.rem(c, cores) == my_core)

        for d in range(2):
            base = tau - (n - 1) - (n - 1 - hops[d])
            c = base - 1 - bits

            @pl.when(my_turn(c))
            def _(d=d, c=c):
                finish(d, c)

            for phase in range(bits - 1, 0, -1):
                c = base - 1 - phase

                @pl.when(my_turn(c))
                def _(d=d, c=c, phase=phase):
                    later_phase(d, c, phase)

            c = base - 1

            @pl.when(my_turn(c))
            def _(d=d, c=c):
                @pl.when(jnp.logical_and(c == my_core, d == first_half()))
                def _():
                    for k in range(1, cores):
                        for t in range(2):
                            send_p(k, t).wait_recv()

                terms(d, c)

        return carry

    def first_half():
        return jnp.where(hops[1] > hops[0], 1, 0)

    lax.fori_loop(0, plan.steps, step, 0)

    for d in range(2):
        @pl.when(hops[d] < n - 1)
        def _(d=d):
            pltpu.make_async_remote_copy(
                src_ref=lossb.at[d], dst_ref=lossb.at[d], send_sem=ls_sem.at[0], recv_sem=lr_sem.at[d],
                device_id={"red": lax.rem(me + 1, n)}, device_id_type=MESH,
            ).wait_recv()

        @pl.when(hops[d] == n - 1)
        def _(d=d):
            for k in range(1, n):
                loss_copy(d, k).wait_send()

        def drain(c, carry, d=d):
            g_store(d, c).wait()

            @pl.when(hops[d] < n - 1)
            def _():
                for t in range(2):
                    rs_copy(d, c, t).wait_send()

            @pl.when(hops[d] > 0)
            def _():
                g_copy(d, c).wait_send()

            @pl.when(hops[d] == n - 1)
            def _():
                for k in range(1, plan.plane):
                    st_copy(c, k).wait_send()

            core = lax.rem(c, cores)

            @pl.when(core != my_core)
            def _():
                x_copy(d, c, lax.rem(my_core - core + cores, cores) - 1, core).wait_send()

            @pl.when(core == my_core)
            def _():
                for phase in range(bits):
                    for s in range(bits):
                        t_copy(d, c // cores, phase, s).wait_send()

            return carry

        lax.fori_loop(0, chunks, drain, 0)
    for k in range(1, cores):
        for t in range(2):
            send_p(k, t).wait_send()
    loss_out[...] = lossb[...]


def on_device(query_lex, query_dense, passage_lex, passage_dense, positives):
    plan = Plan(query_lex, query_dense, passage_lex)
    n, passes, cores, chunks, groups, bits = plan.red, plan.passes, plan.cores, plan.chunks, plan.groups, plan.bits
    tiles = (passes, cores, 2, groups, plan.rows)
    pos = positives.reshape(tiles).transpose(2, 3, 1, 0, 4).reshape(2, chunks, 1, LANES)
    any_space = pl.BlockSpec(memory_space=pl.ANY)
    vmem = pl.BlockSpec(memory_space=pltpu.VMEM)
    dma = pltpu.SemaphoreType.DMA
    grads, loss, gql, gqd = pl.pallas_call(
        functools.partial(fused, plan),
        out_shape=(
            jax.ShapeDtypeStruct((2, chunks, 2, plan.passages, LANES), BF16),
            jax.ShapeDtypeStruct((2, chunks, 8, LANES), F32),
            jax.ShapeDtypeStruct((2, groups, plan.rows, plan.lex), F32),
            jax.ShapeDtypeStruct((2, groups, plan.rows, plan.dense), F32),
        ),
        in_specs=[any_space, any_space, any_space, any_space, vmem],
        out_specs=(any_space, vmem, vmem, vmem),
        scratch_shapes=[
            pltpu.VMEM((2, chunks, passes, plan.rows, plan.lex), BF16),
            pltpu.VMEM((2, chunks, passes, plan.rows, plan.dense), BF16),
            pltpu.VMEM((cores, plan.passages, plan.lex), BF16),
            pltpu.VMEM((cores, plan.passages, plan.dense), BF16),
            pltpu.VMEM((2, chunks, 2, plan.passages, LANES), F32),
            pltpu.VMEM((2, chunks, 2, plan.passages, LANES), BF16),
            pltpu.VMEM((2, groups, max(cores - 1, 1), 2, plan.passages, LANES), BF16),
            pltpu.VMEM((chunks, plan.plane, STAT_ROWS, LANES), F32),
            pltpu.VMEM((2, chunks, 8, LANES), F32),
            pltpu.VMEM((2, groups, passes - 1, plan.rows, plan.columns), BF16),
            pltpu.VMEM((2, groups, passes - 1, plan.rows, plan.columns), BF16),
            pltpu.VMEM((2, plan.keep_slots, passes // 2, plan.rows, plan.columns), F32),
            dma((2, chunks, 2)),
            dma((2,)),
            dma((2, chunks)),
            dma((max(cores - 1, 1), 2)),
            dma((max(cores - 1, 1), 2)),
            dma((2, chunks, 2)),
            dma((2, chunks, 2)),
            dma((chunks, plan.plane - 1)),
            dma((chunks, plan.plane - 1)),
            dma((2, chunks)),
            dma((2, chunks)),
            dma((2, chunks)),
            dma((2, groups, max(cores - 1, 1))),
            dma((2, groups, bits, bits)),
            dma((2, groups, bits, bits)),
            dma((max(n - 1, 1),)),
            dma((2,)),
        ],
        compiler_params=pltpu.CompilerParams(
            collective_id=0, has_side_effects=True, vmem_limit_bytes=67043328
        ),
    )(
        query_lex.reshape(passes, cores, plan.block, plan.lex),
        query_dense.reshape(passes, cores, plan.block, plan.dense),
        passage_lex,
        passage_dense,
        pos,
    )
    own_queries = plan.queries // n
    loss = loss[:, :, 0].reshape(2, groups, cores, passes, plan.rows).transpose(3, 2, 0, 1, 4).reshape(-1)
    loss_rows = lax.dynamic_slice_in_dim(loss, lax.axis_index("red") * own_queries, own_queries)
    whole = grads.reshape(2, groups, cores, 2, plan.passages, passes, plan.rows)
    whole = whole.transpose(3, 4, 5, 2, 0, 1, 6).reshape(2, plan.passages, plan.queries)
    grad_passage_lex = jnp.dot(whole[0], query_lex, preferred_element_type=F32)
    grad_passage_dense = jnp.dot(whole[1], query_dense, preferred_element_type=F32)
    return (
        loss_rows,
        gql.reshape(plan.block, plan.lex),
        gqd.reshape(plan.block, plan.dense),
        grad_passage_lex,
        grad_passage_dense,
    )


def solution(mesh):
    return jax.shard_map(
        on_device,
        mesh=mesh,
        in_specs=(
            P(None, "red"),
            P(None, "red"),
            P(("pass", "grp"), "red"),
            P(("pass", "grp"), "red"),
            P(),
        ),
        out_specs=(
            P("red"),
            P(("pass", "grp"), "red"),
            P(("pass", "grp"), "red"),
            P(("pass", "grp"), "red"),
            P(("pass", "grp"), "red"),
        ),
        check_vma=False,
    )
```

```python
import functools

import jax
import jax.numpy as jnp
from jax import lax
from jax.experimental import pallas as pl
from jax.experimental.pallas import tpu as pltpu
from jax.sharding import PartitionSpec as P

MESH = pl.DeviceIdType.MESH
LANES = 128
HALF = LANES // 2
STAT_ROWS = 8
F32 = jnp.float32
BF16 = jnp.bfloat16


class Plan:
    def __init__(self, query_lex, query_dense, passage_lex):
        self.red = lax.axis_size("red")
        self.passes = lax.axis_size("pass")
        self.cores = lax.axis_size("grp")
        self.queries, self.lex = query_lex.shape
        self.dense = query_dense.shape[1]
        self.passages = passage_lex.shape[0]
        self.block = self.queries // (self.passes * self.cores)
        self.rows = LANES // self.passes
        self.half = self.block // 2
        self.groups = self.half // self.rows
        self.pairs = self.groups * self.cores
        self.chunks = 2 * self.pairs
        self.bits = self.passes.bit_length() - 1
        self.plane = self.passes * self.cores
        self.tile = min(512, self.lex, self.dense)
        self.columns = self.lex + self.dense
        tiles = self.columns // self.tile
        self.edges = [(s * tiles // self.bits) * self.tile for s in range(self.bits)] + [self.columns]
        self.lag = 2
        self.keep_slots = -(-self.bits * self.lag // (2 * self.cores))
        self.parts = 2
        assert self.passes == 1 << self.bits and self.passes > 1
        assert self.groups * self.rows * 2 == self.block
        assert self.lex % self.tile == 0 and self.dense % self.tile == 0
        self.steps = self.chunks + 2 * self.red + self.bits * self.lag


def fused(
    plan,
    ql_hbm, qd_hbm, pl_hbm, pd_hbm, pos_ref,
    loss_out, gql_out, gqd_out, left_out, qlp_out, qdp_out,
    qlv, qdv, plv, pdv, rs, own, grad, left, gx, st, lossb, tsend, trecv, keep,
    q_sem, p_sem, o_sem, w_sem, ps_sem, pr_sem, rss_sem, rsr_sem, sts_sem, str_sem, gs_sem, gr_sem,
    xs_sem, xr_sem, ts_sem, tr_sem, ls_sem, lr_sem,
):
    n, passes, cores, chunks, bits = plan.red, plan.passes, plan.cores, plan.chunks, plan.bits
    pairs = plan.pairs
    me = lax.axis_index("red")
    my_pass = lax.axis_index("pass")
    my_core = lax.axis_index("grp")
    place = my_pass * cores + my_core
    hops = (n - 1 - me, me)
    onward = (me - 1, me + 1)
    back = (me + 1, me - 1)

    def local_q(d, c, t):
        core, group = lax.rem(c, cores), c // cores
        source = (ql_hbm, qd_hbm)[t]
        target = (qlv, qdv)[t]
        start = d * plan.half + group * plan.rows
        return pltpu.make_async_copy(
            source.at[:, core, pl.ds(pl.multiple_of(start, plan.rows), plan.rows), :],
            target.at[d, c],
            q_sem.at[d, c, t],
        )

    def local_p(t):
        return pltpu.make_async_copy((pl_hbm, pd_hbm)[t], (plv, pdv)[t].at[my_core], p_sem.at[t])

    def send_p(k, t):
        other = lax.rem(my_core + k, cores)
        return pltpu.make_async_remote_copy(
            src_ref=(pl_hbm, pd_hbm)[t],
            dst_ref=(plv, pdv)[t].at[my_core],
            send_sem=ps_sem.at[k - 1, t],
            recv_sem=pr_sem.at[k - 1, t],
            device_id={"grp": other},
            device_id_type=MESH,
        )

    def rs_copy(d, u, part):
        size = plan.passages // plan.parts
        where = (d, u, pl.ds(part * size, size))
        return pltpu.make_async_remote_copy(
            src_ref=rs.at[where],
            dst_ref=rs.at[where],
            send_sem=rss_sem.at[d, u, part],
            recv_sem=rsr_sem.at[d, u, part],
            device_id={"red": onward[d]},
            device_id_type=MESH,
        )

    def st_copy(c, k):
        peer = lax.rem(place + k, plan.plane)
        return pltpu.make_async_remote_copy(
            src_ref=st.at[c, place],
            dst_ref=st.at[c, place],
            send_sem=sts_sem.at[c, k - 1],
            recv_sem=str_sem.at[c, k - 1],
            device_id={"pass": peer // cores, "grp": lax.rem(peer, cores)},
            device_id_type=MESH,
        )

    def g_copy(d, c):
        return pltpu.make_async_remote_copy(
            src_ref=grad.at[d, c],
            dst_ref=grad.at[d, c],
            send_sem=gs_sem.at[d, c],
            recv_sem=gr_sem.at[d, c],
            device_id={"red": back[d]},
            device_id_type=MESH,
        )

    def left_store(d, c):
        where = pl.ds(pl.multiple_of((d * pairs + c) * LANES, LANES), LANES)
        return pltpu.make_async_copy(left.at[:, :, where], left_out.at[:, :, where], o_sem.at[d, c])

    def q_store(d, c, t):
        return pltpu.make_async_copy((qlv, qdv)[t].at[d, c], (qlp_out, qdp_out)[t].at[d, c], w_sem.at[d, c, t])

    def x_copy(d, u, slot, target):
        group = u // (2 * cores)
        return pltpu.make_async_remote_copy(
            src_ref=grad.at[d, u],
            dst_ref=gx.at[d, group, lax.rem(u, 2), slot],
            send_sem=xs_sem.at[d, u],
            recv_sem=xr_sem.at[d, group, lax.rem(u, 2), slot],
            device_id={"grp": target},
            device_id_type=MESH,
        )

    def part(phase):
        start = passes - (passes >> phase)
        return start, passes >> (phase + 1)

    def t_copy(d, group, phase, s):
        first, count = part(phase)
        lo, hi = plan.edges[s], plan.edges[s + 1]
        bit = (s + phase) % bits
        mine = lax.rem(my_pass // (1 << bit), 2)
        peer = my_pass + (1 - 2 * mine) * (1 << bit)
        where = (d, group, pl.ds(first, count), slice(None), pl.ds(lo, hi - lo))
        return pltpu.make_async_remote_copy(
            src_ref=tsend.at[where],
            dst_ref=trecv.at[where],
            send_sem=ts_sem.at[d, group, phase, s],
            recv_sem=tr_sem.at[d, group, phase, s],
            device_id={"pass": peer},
            device_id_type=MESH,
        )

    def loss_copy(d, k):
        return pltpu.make_async_remote_copy(
            src_ref=lossb.at[d],
            dst_ref=lossb.at[d],
            send_sem=ls_sem.at[k - 1],
            recv_sem=lr_sem.at[d],
            device_id={"red": lax.rem(me + k, n)},
            device_id_type=MESH,
        )

    for t in range(2):
        local_p(t).start()
    for d in range(2):
        for t in range(2):
            local_q(d, 0, t).start()

    barrier = pltpu.get_barrier_semaphore()
    for k in range(1, plan.plane):
        peer = lax.rem(place + k, plan.plane)
        pl.semaphore_signal(
            barrier, inc=1,
            device_id={"pass": peer // cores, "grp": lax.rem(peer, cores)}, device_id_type=MESH,
        )
    for k in range(1, n):
        pl.semaphore_signal(barrier, inc=1, device_id={"red": lax.rem(me + k, n)}, device_id_type=MESH)
    pl.semaphore_wait(barrier, plan.plane - 1 + n - 1)

    for t in range(2):
        local_p(t).wait()
    for c in range(1, pairs):
        for d in range(2):
            for t in range(2):
                local_q(d, c, t).start()
    for k in range(1, cores):
        for t in range(2):
            send_p(k, t).start()

    first_column = place * plan.passages
    column = first_column + lax.broadcasted_iota(jnp.int32, (plan.passages, LANES), 0)

    low = lax.broadcasted_iota(jnp.int32, (plan.passages, LANES), 1) < HALF
    low_row = lax.broadcasted_iota(jnp.int32, (1, LANES), 1) < HALF

    def swap(values):
        return pltpu.roll(values, HALF, 1)

    def own_scores(d, c):
        totals = []
        for t in range(2):
            local_q(d, c, t).wait()
            q_store(d, c, t).start()
            rows = (qlv, qdv)[t][d, c].reshape(LANES, (plan.lex, plan.dense)[t])
            totals.append(lax.dot_general(
                (plv, pdv)[t][my_core], rows, (((1,), (1,)), ((), ())), preferred_element_type=F32
            ))
        lexical, dense = totals
        own[d, 0] = jnp.where(low, lexical, swap(dense))
        own[d, 1] = jnp.where(low, swap(lexical), dense)

    def add_scores(d, u, part):
        size = plan.passages // plan.parts
        where = pl.ds(part * size, size)
        mine = own.at[d, lax.rem(u, 2), where]
        rs_now = rs.at[d, u, where]

        @pl.when(hops[d] > 0)
        def _():
            rs_copy(d, u, part).wait_recv()
            rs_now[...] += mine[...]

        @pl.when(hops[d] == 0)
        def _():
            rs_now[...] = mine[...]

        @pl.when(hops[d] < n - 1)
        def _():
            rs_copy(d, u, part).start()

    def joined_of(scores):
        other = swap(scores)
        return jnp.where(low, other + 0.3 * scores, scores + 0.3 * other)

    def statistics(d, u):
        scores = rs[d, u]
        joined = joined_of(scores)
        target = column == pos_ref[d, u]
        st_now = st.at[u, place]
        largest = jnp.max(scores, axis=0, keepdims=True)
        largest_joined = jnp.max(joined, axis=0, keepdims=True)
        power = jnp.exp(joined - largest_joined)
        st_now[0:1] = largest
        st_now[1:2] = largest_joined
        st_now[2:3] = jnp.sum(jnp.exp(scores - largest), axis=0, keepdims=True)
        st_now[3:4] = jnp.sum(power, axis=0, keepdims=True)
        st_now[4:5] = jnp.sum(power * (joined - scores), axis=0, keepdims=True)
        st_now[5:6] = jnp.sum(jnp.where(target, scores, 0.0), axis=0, keepdims=True)
        st_now[6:7] = jnp.sum(jnp.where(target, joined, 0.0), axis=0, keepdims=True)
        st_now[7:8] = jnp.zeros((1, LANES), F32)
        for k in range(1, plan.plane):
            st_copy(u, k).start()

    def gradients(d, u):
        for k in range(1, plan.plane):
            st_copy(u, k).wait_recv()
        everyone = st[u]
        maxima = jnp.max(everyone[:, 0:2], axis=0)
        factors = jnp.exp(everyone[:, 0:2] - maxima[None])
        totals = jnp.sum(factors * everyone[:, 2:4], axis=0)
        weighted = jnp.sum(factors[:, 1:2] * everyone[:, 4:5], axis=0)
        picked = jnp.sum(everyone[:, 5:7], axis=0)
        logs = maxima + jnp.log(totals)
        log_own, log_joined = logs[0:1], logs[1:2]
        divergence = weighted / totals[1:2] - log_joined + log_own
        share = 0.5 * (log_own - picked[0:1]) + 0.5 * divergence
        loss = (log_joined - picked[1:2]) + (share + swap(share))
        lossb[d, u] = jnp.broadcast_to(loss, (8, LANES))
        scores = rs[d, u]
        joined = joined_of(scores)
        prob = jnp.where(low_row, -0.2, 0.5) * jnp.exp(joined - log_joined) + jnp.exp(scores - log_own)
        hit = jnp.where(column == pos_ref[d, u], jnp.where(low_row, 0.8, 1.5), 0.0)
        grad[d, u] = (prob - hit).astype(BF16)

    def terms(d, c):
        group = c // cores
        slot = lax.rem(group, plan.keep_slots)
        turned = [(my_core, [grad[d, 2 * c + h].T for h in range(2)])]
        for k in range(1, cores):
            core = lax.rem(my_core + k, cores)
            for h in range(2):
                x_copy(d, 2 * c + h, k - 1, core).wait_recv()
            turned.append((core, [gx[d, group, h, k - 1].T for h in range(2)]))
        for t in range(2):
            base = 0 if t == 0 else plan.lex
            lefts = [
                (core, jnp.concatenate([half[t * HALF:(t + 1) * HALF] for half in halves], axis=0))
                for core, halves in turned
            ]
            width = (plan.lex, plan.dense)[t]
            for s in range(bits):
                lo = max(plan.edges[s], base)
                hi = min(plan.edges[s + 1], base + width)
                if lo >= hi:
                    continue

                def column_tile(i, carry, lo=lo, s=s, t=t, base=base, lefts=lefts):
                    where = pl.ds(pl.multiple_of(lo - base + i * plan.tile, plan.tile), plan.tile)
                    there = pl.ds(pl.multiple_of(lo + i * plan.tile, plan.tile), plan.tile)
                    total = None
                    for core, left in lefts:
                        term = jnp.dot(left, (plv, pdv)[t][core, :, where], preferred_element_type=F32)
                        total = term if total is None else total + term
                    blocks = total.reshape(passes, plan.rows, plan.tile)
                    bit = s % bits
                    split = blocks.reshape(passes >> (bit + 1), 2, 1 << bit, plan.rows, plan.tile)
                    mine = lax.rem(my_pass // (1 << bit), 2)
                    zero, one = split[:, 0], split[:, 1]
                    pick = mine == 0
                    kept = jnp.where(pick, zero, one).reshape(passes // 2, plan.rows, plan.tile)
                    away = jnp.where(pick, one, zero).reshape(passes // 2, plan.rows, plan.tile)
                    first, count = part(0)
                    for a in range(count):
                        source = order(s, a)
                        tsend[d, group, first + a, :, there] = away[source].astype(BF16)
                        keep[d, slot, a, :, there] = kept[source]
                    return carry

                lax.fori_loop(0, (hi - lo) // plan.tile, column_tile, 0)
        for s in range(bits):
            t_copy(d, group, 0, s).start()

    def order(s, a):
        first_bit = s % bits
        natural = [bit for bit in range(bits) if bit != first_bit]
        place_of = 0
        for step in range(1, bits):
            bit = (s + step) % bits
            place_of |= ((a >> (step - 1)) & 1) << natural.index(bit)
        return place_of

    def later_phase(d, c, phase):
        group = c // cores
        slot = lax.rem(group, plan.keep_slots)
        for s in range(bits):
            t_copy(d, group, phase - 1, s).wait_recv()
            lo, hi = plan.edges[s], plan.edges[s + 1]
            before, had = part(phase - 1)
            first, count = part(phase)
            bit = (s + phase) % bits
            mine = lax.rem(my_pass // (1 << bit), 2)

            def column_tile(i, carry, lo=lo, before=before, first=first, count=count, mine=mine):
                there = pl.ds(pl.multiple_of(lo + i * plan.tile, plan.tile), plan.tile)
                for a in range(count):
                    both = []
                    for value in range(2):
                        b = 2 * a + value
                        both.append(keep[d, slot, b, :, there] + trecv[d, group, before + b, :, there].astype(F32))
                    pick = mine == 0
                    tsend[d, group, first + a, :, there] = jnp.where(pick, both[1], both[0]).astype(BF16)
                    keep[d, slot, a, :, there] = jnp.where(pick, both[0], both[1])
                return carry

            lax.fori_loop(0, (hi - lo) // plan.tile, column_tile, 0)
            t_copy(d, group, phase, s).start()

    def finish(d, c):
        group = c // cores
        slot = lax.rem(group, plan.keep_slots)
        last, _ = part(bits - 1)
        for s in range(bits):
            t_copy(d, group, bits - 1, s).wait_recv()
        for out, base, width in ((gql_out, 0, plan.lex), (gqd_out, plan.lex, plan.dense)):

            def column_tile(i, carry, out=out, base=base):
                there = pl.ds(pl.multiple_of(base + i * plan.tile, plan.tile), plan.tile)
                where = pl.ds(pl.multiple_of(i * plan.tile, plan.tile), plan.tile)
                out[d, group, :, where] = keep[d, slot, 0, :, there] + trecv[d, group, last, :, there].astype(F32)
                return carry

            lax.fori_loop(0, width // plan.tile, column_tile, 0)

    def lay_out(d, c):
        halves = [grad[d, 2 * c + h].astype(F32) for h in range(2)]
        where = pl.ds(pl.multiple_of((d * pairs + c) * LANES, LANES), LANES)
        left[0, :, where] = jnp.where(low, halves[0], swap(halves[1])).astype(BF16)
        left[1, :, where] = jnp.where(low, swap(halves[0]), halves[1]).astype(BF16)
        left_store(d, c).start()

    def inside(u):
        return jnp.logical_and(u >= 0, u < chunks)

    def step(tau, carry):
        def my_turn(u):
            return jnp.logical_and(
                inside(u), jnp.logical_and(lax.rem(u, 2) == 1, lax.rem(u // 2, cores) == my_core)
            )

        for d in range(2):
            base = tau - (n - 1) - 2 - (n - 1 - hops[d])
            u = base - plan.lag * bits

            @pl.when(my_turn(u))
            def _(d=d, u=u):
                finish(d, u // 2)

            for phase in range(bits - 1, 0, -1):
                u = base - plan.lag * phase

                @pl.when(my_turn(u))
                def _(d=d, u=u, phase=phase):
                    later_phase(d, u // 2, phase)

            @pl.when(my_turn(base))
            def _(d=d, u=base):
                c = u // 2

                @pl.when(jnp.logical_and(c == my_core, d == first_half()))
                def _():
                    for k in range(1, cores):
                        for t in range(2):
                            send_p(k, t).wait_recv()

                terms(d, c)

        for part in range(plan.parts):
            for d in range(2):
                u = tau - hops[d]
                if part == 0:
                    @pl.when(jnp.logical_and(inside(u), lax.rem(u, 2) == 0))
                    def _(d=d, u=u):
                        own_scores(d, u // 2)

                @pl.when(inside(u))
                def _(d=d, u=u, part=part):
                    add_scores(d, u, part)

        for d in range(2):
            u = tau - (n - 1) - 1

            @pl.when(jnp.logical_and(inside(u), hops[d] == n - 1))
            def _(d=d, u=u):
                gradients(d, u)

                @pl.when(u == chunks - 1)
                def _():
                    for k in range(1, n):
                        loss_copy(d, k).start()

        for d in range(2):
            u = tau - (n - 1)

            @pl.when(jnp.logical_and(inside(u), hops[d] == n - 1))
            def _(d=d, u=u):
                statistics(d, u)

        for d in range(2):
            away = n - 1 - hops[d]
            u = tau - (n - 1) - 1 - away

            @pl.when(inside(u))
            def _(d=d, u=u, away=away):
                @pl.when(away > 0)
                def _():
                    g_copy(d, u).wait_recv()

                @pl.when(away < n - 1)
                def _():
                    g_copy(d, u).start()

                core = lax.rem(u // 2, cores)

                @pl.when(core != my_core)
                def _():
                    x_copy(d, u, lax.rem(my_core - core + cores, cores) - 1, core).start()

                @pl.when(lax.rem(u, 2) == 1)
                def _():
                    lay_out(d, u // 2)

        return carry

    def first_half():
        return jnp.where(hops[1] > hops[0], 1, 0)

    lax.fori_loop(0, plan.steps, step, 0)

    for d in range(2):
        @pl.when(hops[d] < n - 1)
        def _(d=d):
            pltpu.make_async_remote_copy(
                src_ref=lossb.at[d], dst_ref=lossb.at[d], send_sem=ls_sem.at[0], recv_sem=lr_sem.at[d],
                device_id={"red": lax.rem(me + 1, n)}, device_id_type=MESH,
            ).wait_recv()

        @pl.when(hops[d] == n - 1)
        def _(d=d):
            for k in range(1, n):
                loss_copy(d, k).wait_send()

        def drain(c, carry, d=d):
            @pl.when(hops[d] < n - 1)
            def _():
                for part in range(plan.parts):
                    rs_copy(d, c, part).wait_send()

            @pl.when(hops[d] > 0)
            def _():
                g_copy(d, c).wait_send()

            @pl.when(hops[d] == n - 1)
            def _():
                for k in range(1, plan.plane):
                    st_copy(c, k).wait_send()

            core = lax.rem(c // 2, cores)

            @pl.when(core != my_core)
            def _():
                x_copy(d, c, lax.rem(my_core - core + cores, cores) - 1, core).wait_send()

            @pl.when(jnp.logical_and(core == my_core, lax.rem(c, 2) == 1))
            def _():
                for phase in range(bits):
                    for s in range(bits):
                        t_copy(d, c // (2 * cores), phase, s).wait_send()

            return carry

        lax.fori_loop(0, chunks, drain, 0)
    for k in range(1, cores):
        for t in range(2):
            send_p(k, t).wait_send()
    for d in range(2):
        for c in range(pairs):
            left_store(d, c).wait()
            for t in range(2):
                q_store(d, c, t).wait()
    loss_out[...] = lossb[...]


def on_device(query_lex, query_dense, passage_lex, passage_dense, positives):
    plan = Plan(query_lex, query_dense, passage_lex)
    n, passes, cores, chunks, groups, bits = plan.red, plan.passes, plan.cores, plan.chunks, plan.groups, plan.bits
    pos = positives.reshape(passes, cores, 2, groups, plan.rows).transpose(2, 3, 1, 0, 4).reshape(2, chunks, 1, HALF)
    pos = jnp.concatenate([pos, pos], axis=-1)
    any_space = pl.BlockSpec(memory_space=pl.ANY)
    vmem = pl.BlockSpec(memory_space=pltpu.VMEM)
    dma = pltpu.SemaphoreType.DMA
    others = max(cores - 1, 1)
    lex_rows = query_lex.reshape(passes, cores, plan.block, plan.lex)
    dense_rows = query_dense.reshape(passes, cores, plan.block, plan.dense)
    loss, gql, gqd, left, lex_ordered, dense_ordered = pl.pallas_call(
        functools.partial(fused, plan),
        out_shape=(
            jax.ShapeDtypeStruct((2, chunks, 8, LANES), F32),
            jax.ShapeDtypeStruct((2, groups, plan.rows, plan.lex), F32),
            jax.ShapeDtypeStruct((2, groups, plan.rows, plan.dense), F32),
            jax.ShapeDtypeStruct((2, plan.passages, plan.queries), BF16),
            jax.ShapeDtypeStruct((2, plan.pairs, passes, plan.rows, plan.lex), BF16),
            jax.ShapeDtypeStruct((2, plan.pairs, passes, plan.rows, plan.dense), BF16),
        ),
        in_specs=[any_space, any_space, any_space, any_space, vmem],
        out_specs=(vmem, vmem, vmem, any_space, any_space, any_space),
        scratch_shapes=[
            pltpu.VMEM((2, plan.pairs, passes, plan.rows, plan.lex), BF16),
            pltpu.VMEM((2, plan.pairs, passes, plan.rows, plan.dense), BF16),
            pltpu.VMEM((cores, plan.passages, plan.lex), BF16),
            pltpu.VMEM((cores, plan.passages, plan.dense), BF16),
            pltpu.VMEM((2, chunks, plan.passages, LANES), F32),
            pltpu.VMEM((2, 2, plan.passages, LANES), F32),
            pltpu.VMEM((2, chunks, plan.passages, LANES), BF16),
            pltpu.VMEM((2, plan.passages, plan.queries), BF16),
            pltpu.VMEM((2, groups, 2, others, plan.passages, LANES), BF16),
            pltpu.VMEM((chunks, plan.plane, STAT_ROWS, LANES), F32),
            pltpu.VMEM((2, chunks, 8, LANES), F32),
            pltpu.VMEM((2, groups, passes - 1, plan.rows, plan.columns), BF16),
            pltpu.VMEM((2, groups, passes - 1, plan.rows, plan.columns), BF16),
            pltpu.VMEM((2, plan.keep_slots, passes // 2, plan.rows, plan.columns), F32),
            dma((2, plan.pairs, 2)),
            dma((2,)),
            dma((2, plan.pairs)),
            dma((2, plan.pairs, 2)),
            dma((others, 2)),
            dma((others, 2)),
            dma((2, chunks, plan.parts)),
            dma((2, chunks, plan.parts)),
            dma((chunks, plan.plane - 1)),
            dma((chunks, plan.plane - 1)),
            dma((2, chunks)),
            dma((2, chunks)),
            dma((2, chunks)),
            dma((2, groups, 2, others)),
            dma((2, groups, bits, bits)),
            dma((2, groups, bits, bits)),
            dma((max(n - 1, 1),)),
            dma((2,)),
        ],
        compiler_params=pltpu.CompilerParams(
            collective_id=0, has_side_effects=True, vmem_limit_bytes=67043328
        ),
    )(lex_rows, dense_rows, passage_lex, passage_dense, pos)
    own_queries = plan.queries // n
    loss = loss[:, :, 0, :HALF].reshape(2, groups, cores, passes, plan.rows).transpose(3, 2, 0, 1, 4).reshape(-1)
    loss_rows = lax.dynamic_slice_in_dim(loss, lax.axis_index("red") * own_queries, own_queries)
    grad_passage_lex, grad_passage_dense = (
        jnp.dot(left[t], rows.reshape(plan.queries, -1), preferred_element_type=F32)
        for t, rows in enumerate((lex_ordered, dense_ordered))
    )
    return (
        loss_rows,
        gql.reshape(plan.block, plan.lex),
        gqd.reshape(plan.block, plan.dense),
        grad_passage_lex,
        grad_passage_dense,
    )


def solution(mesh):
    return jax.shard_map(
        on_device,
        mesh=mesh,
        in_specs=(
            P(None, "red"),
            P(None, "red"),
            P(("pass", "grp"), "red"),
            P(("pass", "grp"), "red"),
            P(),
        ),
        out_specs=(
            P("red"),
            P(("pass", "grp"), "red"),
            P(("pass", "grp"), "red"),
            P(("pass", "grp"), "red"),
            P(("pass", "grp"), "red"),
        ),
        check_vma=False,
    )
```

```python
import functools

import jax
import jax.numpy as jnp
from jax import lax
from jax.experimental import pallas as pl
from jax.experimental.pallas import tpu as pltpu
from jax.sharding import PartitionSpec as P

MESH = pl.DeviceIdType.MESH
LANES = 128
HALF = LANES // 2
STAT_ROWS = 8
F32 = jnp.float32
BF16 = jnp.bfloat16


class Plan:
    def __init__(self, query_lex, query_dense, passage_lex):
        self.red = lax.axis_size("red")
        self.passes = lax.axis_size("pass")
        self.cores = lax.axis_size("grp")
        self.queries, self.lex = query_lex.shape
        self.dense = query_dense.shape[1]
        self.passages = passage_lex.shape[0]
        self.block = self.queries // (self.passes * self.cores)
        self.rows = LANES // self.passes
        self.half = self.block // 2
        self.groups = self.half // self.rows
        self.pairs = self.groups * self.cores
        self.chunks = 2 * self.pairs
        self.bits = self.passes.bit_length() - 1
        self.plane = self.passes * self.cores
        self.tile = min(512, self.lex, self.dense)
        self.columns = self.lex + self.dense
        tiles = self.columns // self.tile
        self.edges = [(s * tiles // self.bits) * self.tile for s in range(self.bits)] + [self.columns]
        self.lag = 2
        self.keep_slots = -(-self.bits * self.lag // (2 * self.cores))
        self.parts = 4
        self.grad_parts = 2
        self.own_slots = 1 + self.red // 2
        assert self.passes == 1 << self.bits and self.passes > 1
        assert self.groups * self.rows * 2 == self.block
        assert self.lex % self.tile == 0 and self.dense % self.tile == 0
        self.steps = self.chunks + 2 * self.red + self.bits * self.lag


def fused(
    plan,
    ql_hbm, qd_hbm, pl_hbm, pd_hbm, pos_ref,
    loss_out, gql_out, gqd_out, left_lex_out, left_dense_out, qlp_out, qdp_out,
    qlv, qdv, plv, pdv, rs, own, grad, left, gx, st, lossb, tsend, trecv, keep,
    q_sem, p_sem, o_sem, w_sem, ps_sem, pr_sem, rss_sem, rsr_sem, sts_sem, str_sem, gs_sem, gr_sem,
    xs_sem, xr_sem, ts_sem, tr_sem, ls_sem, lr_sem,
):
    n, passes, cores, chunks, bits = plan.red, plan.passes, plan.cores, plan.chunks, plan.bits
    pairs = plan.pairs
    me = lax.axis_index("red")
    my_pass = lax.axis_index("pass")
    my_core = lax.axis_index("grp")
    place = my_pass * cores + my_core
    hops = (n - 1 - me, me)
    onward = (me - 1, me + 1)
    back = (me + 1, me - 1)

    def local_q(d, c, t):
        core, group = lax.rem(c, cores), c // cores
        source = (ql_hbm, qd_hbm)[t]
        target = (qlv, qdv)[t]
        start = d * plan.half + group * plan.rows
        return pltpu.make_async_copy(
            source.at[:, core, pl.ds(pl.multiple_of(start, plan.rows), plan.rows), :],
            target.at[c, d],
            q_sem.at[d, c, t],
        )

    def local_p(t):
        return pltpu.make_async_copy((pl_hbm, pd_hbm)[t], (plv, pdv)[t].at[my_core], p_sem.at[t])

    def send_p(k, t):
        other = lax.rem(my_core + k, cores)
        return pltpu.make_async_remote_copy(
            src_ref=(pl_hbm, pd_hbm)[t],
            dst_ref=(plv, pdv)[t].at[my_core],
            send_sem=ps_sem.at[k - 1, t],
            recv_sem=pr_sem.at[k - 1, t],
            device_id={"grp": other},
            device_id_type=MESH,
        )

    def rs_copy(d, u, part):
        size = plan.passages // plan.parts
        where = (d, u, pl.ds(part * size, size))
        return pltpu.make_async_remote_copy(
            src_ref=rs.at[where],
            dst_ref=rs.at[where],
            send_sem=rss_sem.at[d, u, part],
            recv_sem=rsr_sem.at[d, u, part],
            device_id={"red": onward[d]},
            device_id_type=MESH,
        )

    def st_copy(c, k):
        peer = lax.rem(place + k, plan.plane)
        return pltpu.make_async_remote_copy(
            src_ref=st.at[c, place],
            dst_ref=st.at[c, place],
            send_sem=sts_sem.at[c, k - 1],
            recv_sem=str_sem.at[c, k - 1],
            device_id={"pass": peer // cores, "grp": lax.rem(peer, cores)},
            device_id_type=MESH,
        )

    def g_copy(d, u, part):
        size = plan.passages // plan.grad_parts
        where = (d, u, pl.ds(part * size, size))
        return pltpu.make_async_remote_copy(
            src_ref=grad.at[where],
            dst_ref=grad.at[where],
            send_sem=gs_sem.at[d, u, part],
            recv_sem=gr_sem.at[d, u, part],
            device_id={"red": back[d]},
            device_id_type=MESH,
        )

    def left_store(d, c, t):
        where = pl.ds(pl.multiple_of((d * pairs + c) * LANES, LANES), LANES)
        out = (left_lex_out, left_dense_out)[t]
        return pltpu.make_async_copy(left.at[t, :, where], out.at[:, where], o_sem.at[d, c, t])

    def q_store(d, c, t):
        return pltpu.make_async_copy((qlv, qdv)[t].at[c, d], (qlp_out, qdp_out)[t].at[d, c], w_sem.at[d, c, t])

    def x_copy(d, u, slot, target):
        group = u // (2 * cores)
        return pltpu.make_async_remote_copy(
            src_ref=grad.at[d, u],
            dst_ref=gx.at[d, group, lax.rem(u, 2), slot],
            send_sem=xs_sem.at[d, u],
            recv_sem=xr_sem.at[d, group, lax.rem(u, 2), slot],
            device_id={"grp": target},
            device_id_type=MESH,
        )

    def part(phase):
        start = passes - (passes >> phase)
        return start, passes >> (phase + 1)

    def t_copy(d, group, phase, s):
        first, count = part(phase)
        lo, hi = plan.edges[s], plan.edges[s + 1]
        bit = (s + phase) % bits
        mine = lax.rem(my_pass // (1 << bit), 2)
        peer = my_pass + (1 - 2 * mine) * (1 << bit)
        where = (d, group, pl.ds(first, count), slice(None), pl.ds(lo, hi - lo))
        return pltpu.make_async_remote_copy(
            src_ref=tsend.at[where],
            dst_ref=trecv.at[where],
            send_sem=ts_sem.at[d, group, phase, s],
            recv_sem=tr_sem.at[d, group, phase, s],
            device_id={"pass": peer},
            device_id_type=MESH,
        )

    def loss_copy(d, k):
        return pltpu.make_async_remote_copy(
            src_ref=lossb.at[d],
            dst_ref=lossb.at[d],
            send_sem=ls_sem.at[k - 1],
            recv_sem=lr_sem.at[d],
            device_id={"red": lax.rem(me + k, n)},
            device_id_type=MESH,
        )

    for t in range(2):
        local_p(t).start()
    for d in range(2):
        for t in range(2):
            local_q(d, 0, t).start()

    barrier = pltpu.get_barrier_semaphore()
    for k in range(1, plan.plane):
        peer = lax.rem(place + k, plan.plane)
        pl.semaphore_signal(
            barrier, inc=1,
            device_id={"pass": peer // cores, "grp": lax.rem(peer, cores)}, device_id_type=MESH,
        )
    for k in range(1, n):
        pl.semaphore_signal(barrier, inc=1, device_id={"red": lax.rem(me + k, n)}, device_id_type=MESH)
    pl.semaphore_wait(barrier, plan.plane - 1 + n - 1)

    for t in range(2):
        local_p(t).wait()
    for c in range(1, pairs):
        for d in range(2):
            for t in range(2):
                local_q(d, c, t).start()
    for k in range(1, cores):
        for t in range(2):
            send_p(k, t).start()

    first_column = place * plan.passages
    column = first_column + lax.broadcasted_iota(jnp.int32, (plan.passages, LANES), 0)

    low = lax.broadcasted_iota(jnp.int32, (plan.passages, LANES), 1) < HALF
    low_row = lax.broadcasted_iota(jnp.int32, (1, LANES), 1) < HALF

    def swap(values):
        return pltpu.roll(values, HALF, 1)

    def own_scores(c):
        totals = []
        for t in range(2):
            for d in range(2):
                local_q(d, c, t).wait()
                q_store(d, c, t).start()
            rows = (qlv, qdv)[t][c].reshape(2 * LANES, (plan.lex, plan.dense)[t])
            totals.append(lax.dot_general(
                (plv, pdv)[t][my_core], rows, (((1,), (1,)), ((), ())), preferred_element_type=F32
            ))
        slot = lax.rem(c, plan.own_slots)
        for d in range(2):
            lexical, dense = (total[:, d * LANES:(d + 1) * LANES] for total in totals)
            own[d, slot, 0] = jnp.where(low, lexical, swap(dense))
            own[d, slot, 1] = jnp.where(low, swap(lexical), dense)

    def add_scores(d, u, part):
        size = plan.passages // plan.parts
        where = pl.ds(part * size, size)
        mine = own.at[d, lax.rem(u // 2, plan.own_slots), lax.rem(u, 2), where]
        rs_now = rs.at[d, u, where]

        @pl.when(hops[d] > 0)
        def _():
            rs_copy(d, u, part).wait_recv()
            rs_now[...] += mine[...]

        @pl.when(hops[d] == 0)
        def _():
            rs_now[...] = mine[...]

        @pl.when(hops[d] < n - 1)
        def _():
            rs_copy(d, u, part).start()

    def joined_of(scores):
        other = swap(scores)
        return jnp.where(low, other + 0.3 * scores, scores + 0.3 * other)

    def statistics(d, u):
        scores = rs[d, u]
        joined = joined_of(scores)
        target = column == pos_ref[d, u]
        st_now = st.at[u, place]
        largest = jnp.max(scores, axis=0, keepdims=True)
        largest_joined = jnp.max(joined, axis=0, keepdims=True)
        power = jnp.exp(joined - largest_joined)
        st_now[0:1] = largest
        st_now[1:2] = largest_joined
        st_now[2:3] = jnp.sum(jnp.exp(scores - largest), axis=0, keepdims=True)
        st_now[3:4] = jnp.sum(power, axis=0, keepdims=True)
        st_now[4:5] = jnp.sum(power * (joined - scores), axis=0, keepdims=True)
        st_now[5:6] = jnp.sum(jnp.where(target, scores, 0.0), axis=0, keepdims=True)
        st_now[6:7] = jnp.sum(jnp.where(target, joined, 0.0), axis=0, keepdims=True)
        st_now[7:8] = jnp.zeros((1, LANES), F32)
        for k in range(1, plan.plane):
            st_copy(u, k).start()

    def gradients(d, u):
        for k in range(1, plan.plane):
            st_copy(u, k).wait_recv()
        everyone = st[u]
        maxima = jnp.max(everyone[:, 0:2], axis=0)
        factors = jnp.exp(everyone[:, 0:2] - maxima[None])
        totals = jnp.sum(factors * everyone[:, 2:4], axis=0)
        weighted = jnp.sum(factors[:, 1:2] * everyone[:, 4:5], axis=0)
        picked = jnp.sum(everyone[:, 5:7], axis=0)
        logs = maxima + jnp.log(totals)
        log_own, log_joined = logs[0:1], logs[1:2]
        divergence = weighted / totals[1:2] - log_joined + log_own
        share = 0.5 * (log_own - picked[0:1]) + 0.5 * divergence
        loss = (log_joined - picked[1:2]) + (share + swap(share))
        lossb[d, u] = jnp.broadcast_to(loss, (8, LANES))
        scores = rs[d, u]
        joined = joined_of(scores)
        prob = jnp.where(low_row, -0.2, 0.5) * jnp.exp(joined - log_joined) + jnp.exp(scores - log_own)
        hit = jnp.where(column == pos_ref[d, u], jnp.where(low_row, 0.8, 1.5), 0.0)
        grad[d, u] = (prob - hit).astype(BF16)

    def terms(d, c):
        group = c // cores
        slot = lax.rem(group, plan.keep_slots)
        turned = [(my_core, [grad[d, 2 * c + h].T for h in range(2)])]
        for k in range(1, cores):
            core = lax.rem(my_core + k, cores)
            for h in range(2):
                x_copy(d, 2 * c + h, k - 1, core).wait_recv()
            turned.append((core, [gx[d, group, h, k - 1].T for h in range(2)]))
        for t in range(2):
            base = 0 if t == 0 else plan.lex
            lefts = [
                (core, jnp.concatenate([half[t * HALF:(t + 1) * HALF] for half in halves], axis=0))
                for core, halves in turned
            ]
            width = (plan.lex, plan.dense)[t]
            for s in range(bits):
                lo = max(plan.edges[s], base)
                hi = min(plan.edges[s + 1], base + width)
                if lo >= hi:
                    continue

                def column_tile(i, carry, lo=lo, s=s, t=t, base=base, lefts=lefts):
                    where = pl.ds(pl.multiple_of(lo - base + i * plan.tile, plan.tile), plan.tile)
                    there = pl.ds(pl.multiple_of(lo + i * plan.tile, plan.tile), plan.tile)
                    total = None
                    for core, left in lefts:
                        term = jnp.dot(left, (plv, pdv)[t][core, :, where], preferred_element_type=F32)
                        total = term if total is None else total + term
                    blocks = total.reshape(passes, plan.rows, plan.tile)
                    bit = s % bits
                    split = blocks.reshape(passes >> (bit + 1), 2, 1 << bit, plan.rows, plan.tile)
                    mine = lax.rem(my_pass // (1 << bit), 2)
                    zero, one = split[:, 0], split[:, 1]
                    pick = mine == 0
                    kept = jnp.where(pick, zero, one).reshape(passes // 2, plan.rows, plan.tile)
                    away = jnp.where(pick, one, zero).reshape(passes // 2, plan.rows, plan.tile)
                    first, count = part(0)
                    for a in range(count):
                        source = order(s, a)
                        tsend[d, group, first + a, :, there] = away[source].astype(BF16)
                        keep[d, slot, a, :, there] = kept[source]
                    return carry

                lax.fori_loop(0, (hi - lo) // plan.tile, column_tile, 0)
        for s in range(bits):
            t_copy(d, group, 0, s).start()

    def order(s, a):
        first_bit = s % bits
        natural = [bit for bit in range(bits) if bit != first_bit]
        place_of = 0
        for step in range(1, bits):
            bit = (s + step) % bits
            place_of |= ((a >> (step - 1)) & 1) << natural.index(bit)
        return place_of

    def later_phase(d, c, phase):
        group = c // cores
        slot = lax.rem(group, plan.keep_slots)
        for s in range(bits):
            t_copy(d, group, phase - 1, s).wait_recv()
            lo, hi = plan.edges[s], plan.edges[s + 1]
            before, had = part(phase - 1)
            first, count = part(phase)
            bit = (s + phase) % bits
            mine = lax.rem(my_pass // (1 << bit), 2)

            def column_tile(i, carry, lo=lo, before=before, first=first, count=count, mine=mine):
                there = pl.ds(pl.multiple_of(lo + i * plan.tile, plan.tile), plan.tile)
                for a in range(count):
                    both = []
                    for value in range(2):
                        b = 2 * a + value
                        both.append(keep[d, slot, b, :, there] + trecv[d, group, before + b, :, there].astype(F32))
                    pick = mine == 0
                    tsend[d, group, first + a, :, there] = jnp.where(pick, both[1], both[0]).astype(BF16)
                    keep[d, slot, a, :, there] = jnp.where(pick, both[0], both[1])
                return carry

            lax.fori_loop(0, (hi - lo) // plan.tile, column_tile, 0)
            t_copy(d, group, phase, s).start()

    def finish(d, c):
        group = c // cores
        slot = lax.rem(group, plan.keep_slots)
        last, _ = part(bits - 1)
        for s in range(bits):
            t_copy(d, group, bits - 1, s).wait_recv()
        for out, base, width in ((gql_out, 0, plan.lex), (gqd_out, plan.lex, plan.dense)):

            def column_tile(i, carry, out=out, base=base):
                there = pl.ds(pl.multiple_of(base + i * plan.tile, plan.tile), plan.tile)
                where = pl.ds(pl.multiple_of(i * plan.tile, plan.tile), plan.tile)
                out[d, group, :, where] = keep[d, slot, 0, :, there] + trecv[d, group, last, :, there].astype(F32)
                return carry

            lax.fori_loop(0, width // plan.tile, column_tile, 0)

    def lay_out(d, c):
        halves = [grad[d, 2 * c + h].astype(F32) for h in range(2)]
        where = pl.ds(pl.multiple_of((d * pairs + c) * LANES, LANES), LANES)
        left[0, :, where] = jnp.where(low, halves[0], swap(halves[1])).astype(BF16)
        left[1, :, where] = jnp.where(low, swap(halves[0]), halves[1]).astype(BF16)
        for t in range(2):
            left_store(d, c, t).start()

    def inside(u):
        return jnp.logical_and(u >= 0, u < chunks)

    def step(tau, carry):
        def my_turn(u):
            return jnp.logical_and(
                inside(u), jnp.logical_and(lax.rem(u, 2) == 1, lax.rem(u // 2, cores) == my_core)
            )

        for d in range(2):
            base = tau - (n - 1) - 2 - (n - 1 - hops[d])
            u = base - plan.lag * bits

            @pl.when(my_turn(u))
            def _(d=d, u=u):
                finish(d, u // 2)

            for phase in range(bits - 1, 0, -1):
                u = base - plan.lag * phase

                @pl.when(my_turn(u))
                def _(d=d, u=u, phase=phase):
                    later_phase(d, u // 2, phase)

            @pl.when(my_turn(base))
            def _(d=d, u=base):
                c = u // 2

                @pl.when(jnp.logical_and(c == my_core, d == first_half()))
                def _():
                    for k in range(1, cores):
                        for t in range(2):
                            send_p(k, t).wait_recv()

                terms(d, c)

        soonest = tau - jnp.minimum(hops[0], hops[1])

        @pl.when(jnp.logical_and(inside(soonest), lax.rem(soonest, 2) == 0))
        def _():
            own_scores(soonest // 2)

        for part in range(plan.parts):
            for d in range(2):
                u = tau - hops[d]
                @pl.when(inside(u))
                def _(d=d, u=u, part=part):
                    add_scores(d, u, part)

        for d in range(2):
            u = tau - (n - 1) - 1

            @pl.when(jnp.logical_and(inside(u), hops[d] == n - 1))
            def _(d=d, u=u):
                gradients(d, u)

                @pl.when(u == chunks - 1)
                def _():
                    for k in range(1, n):
                        loss_copy(d, k).start()

        for d in range(2):
            u = tau - (n - 1)

            @pl.when(jnp.logical_and(inside(u), hops[d] == n - 1))
            def _(d=d, u=u):
                statistics(d, u)

        for d in range(2):
            away = n - 1 - hops[d]
            u = tau - (n - 1) - 1 - away

            @pl.when(inside(u))
            def _(d=d, u=u, away=away):
                for part in range(plan.grad_parts):
                    @pl.when(away > 0)
                    def _(part=part):
                        g_copy(d, u, part).wait_recv()

                    @pl.when(away < n - 1)
                    def _(part=part):
                        g_copy(d, u, part).start()

                core = lax.rem(u // 2, cores)

                @pl.when(core != my_core)
                def _():
                    x_copy(d, u, lax.rem(my_core - core + cores, cores) - 1, core).start()

                @pl.when(lax.rem(u, 2) == 1)
                def _():
                    lay_out(d, u // 2)

        return carry

    def first_half():
        return jnp.where(hops[1] > hops[0], 1, 0)

    lax.fori_loop(0, plan.steps, step, 0)

    for d in range(2):
        @pl.when(hops[d] < n - 1)
        def _(d=d):
            pltpu.make_async_remote_copy(
                src_ref=lossb.at[d], dst_ref=lossb.at[d], send_sem=ls_sem.at[0], recv_sem=lr_sem.at[d],
                device_id={"red": lax.rem(me + 1, n)}, device_id_type=MESH,
            ).wait_recv()

        @pl.when(hops[d] == n - 1)
        def _(d=d):
            for k in range(1, n):
                loss_copy(d, k).wait_send()

        def drain(c, carry, d=d):
            @pl.when(hops[d] < n - 1)
            def _():
                for part in range(plan.parts):
                    rs_copy(d, c, part).wait_send()

            @pl.when(hops[d] > 0)
            def _():
                for part in range(plan.grad_parts):
                    g_copy(d, c, part).wait_send()

            @pl.when(hops[d] == n - 1)
            def _():
                for k in range(1, plan.plane):
                    st_copy(c, k).wait_send()

            core = lax.rem(c // 2, cores)

            @pl.when(core != my_core)
            def _():
                x_copy(d, c, lax.rem(my_core - core + cores, cores) - 1, core).wait_send()

            @pl.when(jnp.logical_and(core == my_core, lax.rem(c, 2) == 1))
            def _():
                for phase in range(bits):
                    for s in range(bits):
                        t_copy(d, c // (2 * cores), phase, s).wait_send()

            return carry

        lax.fori_loop(0, chunks, drain, 0)
    for k in range(1, cores):
        for t in range(2):
            send_p(k, t).wait_send()
    for d in range(2):
        for c in range(pairs):
            for t in range(2):
                left_store(d, c, t).wait()
                q_store(d, c, t).wait()
    loss_out[...] = lossb[...]


def on_device(query_lex, query_dense, passage_lex, passage_dense, positives):
    plan = Plan(query_lex, query_dense, passage_lex)
    n, passes, cores, chunks, groups, bits = plan.red, plan.passes, plan.cores, plan.chunks, plan.groups, plan.bits
    pos = positives.reshape(passes, cores, 2, groups, plan.rows).transpose(2, 3, 1, 0, 4).reshape(2, chunks, 1, HALF)
    pos = jnp.concatenate([pos, pos], axis=-1)
    any_space = pl.BlockSpec(memory_space=pl.ANY)
    vmem = pl.BlockSpec(memory_space=pltpu.VMEM)
    dma = pltpu.SemaphoreType.DMA
    others = max(cores - 1, 1)
    lex_rows = query_lex.reshape(passes, cores, plan.block, plan.lex)
    dense_rows = query_dense.reshape(passes, cores, plan.block, plan.dense)
    loss, gql, gqd, left_lex, left_dense, lex_ordered, dense_ordered = pl.pallas_call(
        functools.partial(fused, plan),
        out_shape=(
            jax.ShapeDtypeStruct((2, chunks, 8, LANES), F32),
            jax.ShapeDtypeStruct((2, groups, plan.rows, plan.lex), F32),
            jax.ShapeDtypeStruct((2, groups, plan.rows, plan.dense), F32),
            jax.ShapeDtypeStruct((plan.passages, plan.queries), BF16),
            jax.ShapeDtypeStruct((plan.passages, plan.queries), BF16),
            jax.ShapeDtypeStruct((2, plan.pairs, passes, plan.rows, plan.lex), BF16),
            jax.ShapeDtypeStruct((2, plan.pairs, passes, plan.rows, plan.dense), BF16),
        ),
        in_specs=[any_space, any_space, any_space, any_space, vmem],
        out_specs=(vmem, vmem, vmem, any_space, any_space, any_space, any_space),
        scratch_shapes=[
            pltpu.VMEM((plan.pairs, 2, passes, plan.rows, plan.lex), BF16),
            pltpu.VMEM((plan.pairs, 2, passes, plan.rows, plan.dense), BF16),
            pltpu.VMEM((cores, plan.passages, plan.lex), BF16),
            pltpu.VMEM((cores, plan.passages, plan.dense), BF16),
            pltpu.VMEM((2, chunks, plan.passages, LANES), F32),
            pltpu.VMEM((2, plan.own_slots, 2, plan.passages, LANES), F32),
            pltpu.VMEM((2, chunks, plan.passages, LANES), BF16),
            pltpu.VMEM((2, plan.passages, plan.queries), BF16),
            pltpu.VMEM((2, groups, 2, others, plan.passages, LANES), BF16),
            pltpu.VMEM((chunks, plan.plane, STAT_ROWS, LANES), F32),
            pltpu.VMEM((2, chunks, 8, LANES), F32),
            pltpu.VMEM((2, groups, passes - 1, plan.rows, plan.columns), BF16),
            pltpu.VMEM((2, groups, passes - 1, plan.rows, plan.columns), BF16),
            pltpu.VMEM((2, plan.keep_slots, passes // 2, plan.rows, plan.columns), F32),
            dma((2, plan.pairs, 2)),
            dma((2,)),
            dma((2, plan.pairs, 2)),
            dma((2, plan.pairs, 2)),
            dma((others, 2)),
            dma((others, 2)),
            dma((2, chunks, plan.parts)),
            dma((2, chunks, plan.parts)),
            dma((chunks, plan.plane - 1)),
            dma((chunks, plan.plane - 1)),
            dma((2, chunks, plan.grad_parts)),
            dma((2, chunks, plan.grad_parts)),
            dma((2, chunks)),
            dma((2, groups, 2, others)),
            dma((2, groups, bits, bits)),
            dma((2, groups, bits, bits)),
            dma((max(n - 1, 1),)),
            dma((2,)),
        ],
        compiler_params=pltpu.CompilerParams(
            collective_id=0, has_side_effects=True, vmem_limit_bytes=67043328
        ),
    )(lex_rows, dense_rows, passage_lex, passage_dense, pos)
    own_queries = plan.queries // n
    loss = loss[:, :, 0, :HALF].reshape(2, groups, cores, passes, plan.rows).transpose(3, 2, 0, 1, 4).reshape(-1)
    loss_rows = lax.dynamic_slice_in_dim(loss, lax.axis_index("red") * own_queries, own_queries)
    grad_passage_lex, grad_passage_dense = (
        jnp.dot(left, rows.reshape(plan.queries, -1), preferred_element_type=F32)
        for left, rows in ((left_lex, lex_ordered), (left_dense, dense_ordered))
    )
    return (
        loss_rows,
        gql.reshape(plan.block, plan.lex),
        gqd.reshape(plan.block, plan.dense),
        grad_passage_lex,
        grad_passage_dense,
    )


def solution(mesh):
    return jax.shard_map(
        on_device,
        mesh=mesh,
        in_specs=(
            P(None, "red"),
            P(None, "red"),
            P(("pass", "grp"), "red"),
            P(("pass", "grp"), "red"),
            P(),
        ),
        out_specs=(
            P("red"),
            P(("pass", "grp"), "red"),
            P(("pass", "grp"), "red"),
            P(("pass", "grp"), "red"),
            P(("pass", "grp"), "red"),
        ),
        check_vma=False,
    )
```
